32 devices in a mesh: gx: 4 (over x, core), gy: 4 (over z), gz: 2 (over y).
Axes of the slice: x: 2, y: 2, z: 4, core: 2. Of those that a mesh axis runs over, the one named last changes fastest.
Arguments:
- density: float32 [16, 128, 256], P('gx', 'gy', 'gz'), may hold values from 0.5 to 2
- velocity: float32 [3, 16, 128, 256], P(None, 'gx', 'gy', 'gz'), may hold values from -2.5 to 2.5
- pressure: float32 [16, 128, 256], P('gx', 'gy', 'gz'), may hold values from 0.5 to 2
Outputs:
- section_state: float32 [5, 16, 128, 256], P(None, 'gx', 'gy', 'gz')
The draws below stay inside these ranges and needn't reach their ends.
All inputs are finite; a program needn't handle non-finite values.
Results may differ from the reference program's by a relative error of at most 0.0003.
Values sent between devices are 32-bit elements; how exact they have to be, the bound alone decides.
A program may use at most 64 MiB of HBM per device.

```python
import math
import jax
import jax.numpy as jnp
from jax import lax

CX = 4
NX = 16
NY = 128
NZ = 256


def draw_velocity(key, part):
    growth = 1.0 + 2.0 * jnp.arange(NX, dtype=jnp.float32) / NX
    growth = growth[None, :, None, None]
    sample = jnp.clip(jax.random.normal(key, (3, NX, NY, NZ), jnp.float32), -2.5, 2.5)
    return 0.3 * growth * sample


def shard_levels(stream_key, shape, split, least, high):
    loudness = 1.0
    for position, shards_of in split:
        steps = jax.random.uniform(jax.random.fold_in(jax.random.fold_in(stream_key, 6), position), (shards_of,), jnp.float32, least / len(split), high / len(split))
        loudness = loudness * jnp.repeat(jnp.exp(steps), shape[position] // shards_of).reshape((-1,) + (1,) * (len(shape) - 1 - position))
    return loudness


def setup_inputs(seed: int = 0) -> dict:
    keys = jax.random.split(jax.random.key(seed), 4)
    return {
        "density": jnp.clip(jnp.exp(math.log(2.0) - 1.3862944 * jax.random.uniform(keys[0], (NX, NY, NZ), jnp.float32) ** shard_levels(keys[0], (NX, NY, NZ), ((0, 4), (1, 4), (2, 2)), -0.2, 0.2)), 0.5, 2.0),
        "velocity": draw_velocity(jax.random.fold_in(keys[3], 71), 0),
        "pressure": jnp.clip(jnp.exp(math.log(2.0) - 1.3862944 * jax.random.uniform(keys[2], (NX, NY, NZ), jnp.float32) ** shard_levels(keys[2], (NX, NY, NZ), ((0, 4), (1, 4), (2, 2)), -0.2, 0.2)), 0.5, 2.0),
    }


gamma_gas = 1.4
weno_eps = 1e-06
cfl_number = 0.4

def conserved(density, velocity, pressure):
    momenta = density[None] * velocity
    kinetic = 0.5 * density * lax.optimization_barrier(jnp.sum(velocity * velocity, axis=0))
    energy = pressure / (gamma_gas - 1.0) + kinetic
    return jnp.concatenate([density[None], momenta, energy[None]], axis=0)

def wave_speed(density, velocity, pressure):
    sound = jnp.sqrt(gamma_gas * pressure / density)
    return jnp.max(lax.optimization_barrier(jnp.sum(jnp.abs(velocity), axis=0)) + 3.0 * sound)

def combine(coeffs, arrays):
    total = None
    for coeff, array in zip(coeffs, arrays):
        if isinstance(coeff, float) and coeff == 0.0:
            continue
        term = coeff * array
        total = term if total is None else total + term
    return total

def weno_face(values):
    first, second, third, fourth, fifth = values
    cand_left = (2.0 * first - 7.0 * second + 11.0 * third) / 6.0
    cand_middle = (-second + 5.0 * third + 2.0 * fourth) / 6.0
    cand_right = (2.0 * third + 5.0 * fourth - fifth) / 6.0
    smooth_left = 13.0 / 12.0 * (first - 2.0 * second + third) ** 2 + 0.25 * (first - 4.0 * second + 3.0 * third) ** 2
    smooth_middle = 13.0 / 12.0 * (second - 2.0 * third + fourth) ** 2 + 0.25 * (second - fourth) ** 2
    smooth_right = 13.0 / 12.0 * (third - 2.0 * fourth + fifth) ** 2 + 0.25 * (3.0 * third - 4.0 * fourth + fifth) ** 2
    weight_left = 0.1 / (weno_eps + smooth_left) ** 2
    weight_middle = 0.6 / (weno_eps + smooth_middle) ** 2
    weight_right = 0.3 / (weno_eps + smooth_right) ** 2
    return (weight_left * cand_left + weight_middle * cand_middle + weight_right * cand_right) / (weight_left + weight_middle + weight_right)

def direction_flux(padded, field_dim, normal_comp):
    cells = padded.shape[field_dim + 1] - 6
    faces = cells + 1
    density = padded[0]
    energy = padded[4]
    velocity = [padded[1 + member] / density for member in range(3)]
    speed_sq = velocity[0] * velocity[0] + velocity[1] * velocity[1] + velocity[2] * velocity[2]
    pressure = (gamma_gas - 1.0) * (energy - 0.5 * density * speed_sq)
    sound_sq = gamma_gas * pressure / density
    sound = jnp.sqrt(sound_sq)
    enthalpy = (energy + pressure) / density
    normal_vel = velocity[normal_comp]
    others = [member for member in range(3) if member != normal_comp]
    order = [0, 1 + normal_comp, 1 + others[0], 1 + others[1], 4]
    state_perm = [padded[member] for member in order]
    flux_perm = [density * normal_vel, padded[1 + normal_comp] * normal_vel + pressure, padded[1 + others[0]] * normal_vel, padded[1 + others[1]] * normal_vel, (energy + pressure) * normal_vel]
    signal = jnp.abs(normal_vel) + sound

    def window(array, offset):
        return lax.slice_in_dim(array, offset, offset + faces, axis=field_dim)
    root_left = jnp.sqrt(window(density, 2))
    root_right = jnp.sqrt(window(density, 3))
    share_left = root_left / (root_left + root_right)
    share_right = root_right / (root_left + root_right)
    roe_vel = [share_left * window(member, 2) + share_right * window(member, 3) for member in velocity]
    roe_enth = share_left * window(enthalpy, 2) + share_right * window(enthalpy, 3)
    jump_sq = sum(((window(member, 3) - window(member, 2)) ** 2 for member in velocity))
    roe_sound_sq = share_left * window(sound_sq, 2) + share_right * window(sound_sq, 3) + 0.5 * (gamma_gas - 1.0) * share_left * share_right * jump_sq
    roe_sound = jnp.sqrt(roe_sound_sq)
    normal_roe = roe_vel[normal_comp]
    tang_first = roe_vel[others[0]]
    tang_second = roe_vel[others[1]]
    roe_qsq = normal_roe * normal_roe + tang_first * tang_first + tang_second * tang_second
    b_one = (gamma_gas - 1.0) / roe_sound_sq
    b_two = 0.5 * b_one * roe_qsq
    inv_sound = 1.0 / roe_sound
    left_rows = [[0.5 * (b_two + normal_roe * inv_sound), -0.5 * (b_one * normal_roe + inv_sound), -0.5 * b_one * tang_first, -0.5 * b_one * tang_second, 0.5 * b_one], [1.0 - b_two, b_one * normal_roe, b_one * tang_first, b_one * tang_second, -b_one], [-tang_first, 0.0, 1.0, 0.0, 0.0], [-tang_second, 0.0, 0.0, 1.0, 0.0], [0.5 * (b_two - normal_roe * inv_sound), -0.5 * (b_one * normal_roe - inv_sound), -0.5 * b_one * tang_first, -0.5 * b_one * tang_second, 0.5 * b_one]]
    right_rows = [[1.0, 1.0, 0.0, 0.0, 1.0], [normal_roe - roe_sound, normal_roe, 0.0, 0.0, normal_roe + roe_sound], [tang_first, tang_first, 1.0, 0.0, tang_first], [tang_second, tang_second, 0.0, 1.0, tang_second], [roe_enth - normal_roe * roe_sound, 0.5 * roe_qsq, tang_first, tang_second, roe_enth + normal_roe * roe_sound]]
    alpha = window(signal, 0)
    for offset in range(1, 6):
        alpha = jnp.maximum(alpha, window(signal, offset))
    plus_vals = [[None] * 6 for member in range(5)]
    minus_vals = [[None] * 6 for member in range(5)]
    for offset in range(6):
        state_here = [window(member, offset) for member in state_perm]
        flux_here = [window(member, offset) for member in flux_perm]
        for charac in range(5):
            char_state = combine(left_rows[charac], state_here)
            char_flux = combine(left_rows[charac], flux_here)
            plus_vals[charac][offset] = 0.5 * (char_flux + alpha * char_state)
            minus_vals[charac][offset] = 0.5 * (char_flux - alpha * char_state)
    hats = []
    for charac in range(5):
        upwind = weno_face(plus_vals[charac][0:5])
        downwind = weno_face([minus_vals[charac][5], minus_vals[charac][4], minus_vals[charac][3], minus_vals[charac][2], minus_vals[charac][1]])
        hats.append(upwind + downwind)
    face_flux = [None] * 5
    for member in range(5):
        face_flux[order[member]] = combine(right_rows[member], hats)
    result = [lax.slice_in_dim(member, 1, faces, axis=field_dim) - lax.slice_in_dim(member, 0, faces - 1, axis=field_dim) for member in face_flux]
    return jnp.stack(result, axis=0)

def reference(density, velocity, pressure):
    state = conserved(density, velocity, pressure)
    step = cfl_number / wave_speed(density, velocity, pressure)
    padded = jnp.pad(state, ((0, 0), (3, 3), (3, 3), (3, 3)), mode='wrap')

    def slab_update(start):
        piece = lax.dynamic_slice_in_dim(padded, start, CX + 6, axis=1)
        total = direction_flux(piece[:, :, 3:-3, 3:-3], 0, 0)
        total = total + direction_flux(piece[:, 3:-3, :, 3:-3], 1, 1)
        total = total + direction_flux(piece[:, 3:-3, 3:-3, :], 2, 2)
        return total
    starts = jnp.arange(NX // CX, dtype=jnp.int32) * CX
    slabs = lax.map(slab_update, starts)
    total = jnp.moveaxis(slabs, 0, 1).reshape(5, NX, NY, NZ)
    return state - step * total
```

```python
import functools

import jax
import jax.numpy as jnp
from jax import lax
from jax.experimental import pallas as pl
from jax.experimental.pallas import tpu as pltpu
from jax.sharding import PartitionSpec as P

MESH = pl.DeviceIdType.MESH
AXES = ("gx", "gy", "gz")
gamma_gas = 1.4
weno_eps = 1e-06
cfl_number = 0.4
scale = 0.125
eps_outer = 0.75 * 16.0 * scale * scale * weno_eps
eps_inner = 0.75 * 4.0 * scale * scale * weno_eps
ROWS = 8


def rcp(x):
    guess = pl.reciprocal(x, approx=True)
    return guess * (2.0 - x * guess)


def cell_arrays(rho, vn, va, vb, p):
    inv_root = lax.rsqrt(rho)
    root = rho * inv_root
    c2 = gamma_gas * p * (inv_root * inv_root)
    mn, ma, mb = rho * vn, rho * va, rho * vb
    energy = 2.5 * p + 0.5 * (mn * vn + ma * va + mb * vb)
    signal = jnp.abs(vn) + c2 * lax.rsqrt(c2)
    return [
        rho, mn, ma, mb, energy,
        mn * vn + p, ma * vn, mb * vn, (energy + p) * vn,
        root, vn, va, vb, c2, signal,
    ]


def put_cells(ref, row, arrays):
    for k, array in enumerate(arrays):
        ref[k, pl.ds(row, ROWS), :] = array


def weno(d1, d2, d3, d4, eps):
    h2 = (d2 + d2) - d1
    h3 = (d3 + d3) - d4
    e1, e2, e3 = d2 - d1, d3 - d2, d4 - d3
    s2, s3 = 0.75 * d2, 0.75 * d3
    a = (e1 * e1 + s2 * h2) + eps
    b = (e2 * e2 + s2 * d3) + eps
    c = (e3 * e3 + s3 * h3) + eps
    bc, ac, ab = b * c, a * c, a * b
    w0 = bc * bc
    w1 = 6.0 * (ac * ac)
    w2 = 1.5 * (ab * ab)
    den = w0 + w1 + (w2 + w2)
    return (w0 * (h2 - d3) + w2 * (h3 - d2)) * rcp(den)


def face_tile(cells, flux, base, stride, row):
    def load(k, j):
        return cells[k, pl.ds(base + j * stride, ROWS), :]

    sl, sr = load(9, 2), load(9, 3)
    inv = rcp(sl + sr)
    wl, wr = sl * inv, sr * inv
    vl = [load(10 + k, 2) for k in range(3)]
    dv = [load(10 + k, 3) - vl[k] for k in range(3)]
    un, ta, tb = [vl[k] + wr * dv[k] for k in range(3)]
    jump = dv[0] * dv[0] + dv[1] * dv[1] + dv[2] * dv[2]
    c2 = wl * load(13, 2) + wr * load(13, 3) + (0.2 * (wl * wr)) * jump
    ic = lax.rsqrt(c2)
    sound = c2 * ic
    b1 = 0.4 * (ic * ic)
    qh = 0.5 * (un * un + ta * ta + tb * tb)
    enth = 2.5 * c2 + qh
    alpha = load(14, 0)
    for j in range(1, 6):
        alpha = jnp.maximum(alpha, load(14, j))

    state = [[load(k, j) for j in range(6)] for k in range(5)]
    phys = [state[1]] + [[load(k, j) for j in range(6)] for k in range(5, 9)]
    du = [[s[j + 1] - s[j] for j in range(5)] for s in state]
    df = [du[1]] + [[s[j + 1] - s[j] for j in range(5)] for s in phys[1:]]
    au = [[alpha * d for d in s] for s in du]

    def project(r, mn, ma, mb, e):
        s = (un * r - mn) * ic
        z = b1 * (e - un * mn - ta * ma - tb * mb + qh * r)
        return z + s, r - z, ma - ta * r, mb - tb * r, z - s

    plus = [project(*[df[k][j] + au[k][j] for k in range(5)]) for j in range(4)]
    minus = [project(*[df[k][j] - au[k][j] for k in range(5)]) for j in range(1, 5)]
    hats = []
    for k in range(5):
        eps = eps_outer if k in (0, 4) else eps_inner
        up = weno(plus[0][k], plus[1][k], plus[2][k], plus[3][k], eps)
        down = weno(minus[3][k], minus[2][k], minus[1][k], minus[0][k], eps)
        hats.append(up - down)
    lin = []
    for k in range(5):
        centre = 6.0 * (phys[k][2] + phys[k][3]) + (df[k][1] - df[k][3])
        lin.append(centre + ((au[k][1] + au[k][3]) - (au[k][2] + au[k][2])))
    h1, h2, h3, h4, h5 = hats
    h2, h3, h4 = h2 + h2, h3 + h3, h4 + h4
    h15 = h1 + h5
    k5 = sound * (h5 - h1)
    s = h15 + h2
    result = [
        lin[0] + s,
        lin[1] + (un * s + k5),
        lin[2] + (ta * s + h3),
        lin[3] + (tb * s + h4),
        lin[4] + (enth * h15 + un * k5 + qh * h2 + ta * h3 + tb * h4),
    ]
    for k in range(5):
        flux[k, pl.ds(row, ROWS), :] = result[k]


def kernel(
    counts, den, vel, pre, out,
    cx, cy, cz, gx, gy, gz, acc, tz, hx, hy, hz, top, got,
    send_sem, recv_sem, top_send, top_recv,
):
    nx, ny, lanes = den.shape
    nrow = nx * ny
    nz = lanes
    tiles = ny // ROWS
    ypad = ny + 3 * ROWS
    yface = ny + ROWS

    me = [lax.axis_index(a) for a in AXES]
    barrier = pltpu.get_barrier_semaphore()
    peers = []
    for axis, name in enumerate(AXES):
        for k in range(1, counts[axis]):
            peers.append((axis, {name: lax.rem(me[axis] + k, counts[axis])}))
    for _, peer in peers:
        pl.semaphore_signal(barrier, inc=1, device_id=peer, device_id_type=MESH)

    def speed(q, best):
        i, r = q // tiles, pl.multiple_of(lax.rem(q, tiles) * ROWS, ROWS)
        inv_root = lax.rsqrt(den[i, pl.ds(r, ROWS), :])
        c2 = gamma_gas * pre[i, pl.ds(r, ROWS), :] * (inv_root * inv_root)
        total = jnp.abs(vel[0, i, pl.ds(r, ROWS), :]) + jnp.abs(vel[1, i, pl.ds(r, ROWS), :])
        total = total + jnp.abs(vel[2, i, pl.ds(r, ROWS), :])
        return jnp.maximum(best, total + 3.0 * (c2 * lax.rsqrt(c2)))

    top[0] = lax.fori_loop(0, nx * tiles, speed, jnp.zeros((ROWS, lanes), jnp.float32))

    tz[0] = den[...].reshape(nrow, nz).T
    for k in range(3):
        tz[1 + k] = vel[k].reshape(nrow, nz).T
    tz[4] = pre[...].reshape(nrow, nz).T

    pl.semaphore_wait(barrier, len(peers))

    def remote(src, dst, slot, peer):
        copy = pltpu.make_async_remote_copy(
            src_ref=src, dst_ref=dst, send_sem=send_sem.at[slot], recv_sem=recv_sem.at[slot],
            device_id=peer, device_id_type=MESH,
        )
        copy.start()
        return copy

    def send_top(axis):
        copies = []
        for slot, (other, peer) in enumerate(peers):
            if other == axis:
                copy = pltpu.make_async_remote_copy(
                    src_ref=top.at[axis], dst_ref=got.at[slot],
                    send_sem=top_send.at[slot], recv_sem=top_recv.at[slot],
                    device_id=peer, device_id_type=MESH,
                )
                copy.start()
                copies.append((slot, copy))
        return copies

    def take_top(axis, copies):
        best = top[axis]
        for slot, copy in copies:
            copy.wait()
            best = jnp.maximum(best, got[slot])
        top[axis + 1] = best

    def near(axis, way):
        return {AXES[axis]: lax.rem(me[axis] + way + counts[axis], counts[axis])}

    top_x = send_top(0)
    zc = [
        remote(tz.at[:, pl.ds(nz - ROWS, ROWS), :], hz.at[0], 0, near(2, 1)),
        remote(tz.at[:, pl.ds(0, ROWS), :], hz.at[1], 1, near(2, -1)),
    ]
    yc, xc = [], []
    for side, start, way in ((0, ny - ROWS, 1), (1, 0, -1)):
        peer = near(1, way)
        slot = 2 + 3 * side
        yc.append(remote(den.at[:, pl.ds(start, ROWS), :], hy.at[side, 0], slot, peer))
        yc.append(remote(vel.at[:, :, pl.ds(start, ROWS), :], hy.at[side, pl.ds(1, 3)], slot + 1, peer))
        yc.append(remote(pre.at[:, pl.ds(start, ROWS), :], hy.at[side, 4], slot + 2, peer))
    for side, start, way in ((0, nx - 3, 1), (1, 0, -1)):
        peer = near(0, way)
        slot = 8 + 3 * side
        xc.append(remote(den.at[pl.ds(start, 3)], hx.at[side, 0], slot, peer))
        xc.append(remote(vel.at[:, pl.ds(start, 3)], hx.at[side, pl.ds(1, 3)], slot + 1, peer))
        xc.append(remote(pre.at[pl.ds(start, 3)], hx.at[side, 4], slot + 2, peer))

    @pl.loop(0, nz // ROWS)
    def _(t):
        r = pl.multiple_of(t * ROWS, ROWS)
        rho, v1, v2, v3, p = [tz[k, pl.ds(r, ROWS), :] for k in range(5)]
        put_cells(cz, r + ROWS, cell_arrays(scale * rho, v3, v1, v2, scale * p))

    @pl.loop(0, nx * tiles)
    def _(q):
        i, r = q // tiles, pl.multiple_of(lax.rem(q, tiles) * ROWS, ROWS)
        rho = scale * den[i, pl.ds(r, ROWS), :]
        p = scale * pre[i, pl.ds(r, ROWS), :]
        v1, v2, v3 = [vel[k, i, pl.ds(r, ROWS), :] for k in range(3)]
        put_cells(cx, pl.multiple_of(3 * ny + q * ROWS, ROWS), cell_arrays(rho, v1, v2, v3, p))
        put_cells(cy, pl.multiple_of(i * ypad + ROWS + r, ROWS), cell_arrays(rho, v2, v1, v3, p))

    take_top(0, top_x)

    def z_face(t):
        r = pl.multiple_of(t * ROWS, ROWS)
        face_tile(cz, gz, r + 5, 1, r)

    pl.loop(1, nz // ROWS - 1)(z_face)
    top_y = send_top(1)
    for side, row in ((0, 0), (1, nz + ROWS)):
        zc[side].wait()
        rho, v1, v2, v3, p = [hz[side, k] for k in range(5)]
        put_cells(cz, row, cell_arrays(scale * rho, v3, v1, v2, scale * p))

    @pl.loop(0, 3)
    def _(t):
        z_face(jnp.where(t == 0, 0, nz // ROWS - 2 + t))

    for k, field in enumerate((0, 3, 1, 2, 4)):
        acc[field] = (gz[k, pl.ds(1, nz), :] - gz[k, pl.ds(0, nz), :]).T

    take_top(1, top_y)

    for copy in yc:
        copy.wait()
    for side in range(2):
        @pl.loop(0, nx)
        def _(i):
            rho, v1, v2, v3, p = [hy[side, k, i] for k in range(5)]
            row = pl.multiple_of(i * ypad + side * (ny + ROWS), ROWS)
            put_cells(cy, row, cell_arrays(scale * rho, v2, v1, v3, scale * p))

    @pl.loop(0, nx * (tiles + 1))
    def _(q):
        i, t = q // (tiles + 1), lax.rem(q, tiles + 1)
        face_tile(cy, gy, i * ypad + t * ROWS + 5, 1, pl.multiple_of(i * yface + t * ROWS, ROWS))

    top_z = send_top(2)

    for copy in xc:
        copy.wait()
    for side in range(2):
        @pl.loop(0, 3 * tiles)
        def _(q):
            i, r = q // tiles, pl.multiple_of(lax.rem(q, tiles) * ROWS, ROWS)
            rho, v1, v2, v3, p = [hx[side, k, i, pl.ds(r, ROWS), :] for k in range(5)]
            row = pl.multiple_of(side * (nx + 3) * ny + q * ROWS, ROWS)
            put_cells(cx, row, cell_arrays(scale * rho, v1, v2, v3, scale * p))

    @pl.loop(0, (nx + 1) * tiles)
    def _(q):
        r = pl.multiple_of(q * ROWS, ROWS)
        face_tile(cx, gx, r, ny, r)

    take_top(2, top_z)
    largest = jnp.max(top[3], axis=(0, 1), keepdims=True)
    factor = jnp.broadcast_to((cfl_number / (12.0 * scale)) / largest, (ROWS, lanes))

    @pl.loop(0, nx * tiles)
    def _(q):
        i, r = q // tiles, pl.multiple_of(lax.rem(q, tiles) * ROWS, ROWS)
        row = pl.multiple_of(q * ROWS, ROWS)
        yrow = pl.multiple_of(i * yface + r, ROWS)
        for field, k in enumerate((0, 2, 1, 3, 4)):
            total = acc[field, pl.ds(row, ROWS), :]
            total = total + (gy[k, pl.ds(yrow + 1, ROWS), :] - gy[k, pl.ds(yrow, ROWS), :])
            total = total + (gx[field, pl.ds(row + ny, ROWS), :] - gx[field, pl.ds(row, ROWS), :])
            state = cx[field, pl.ds(pl.multiple_of(row + 3 * ny, ROWS), ROWS), :]
            out[field, i, pl.ds(r, ROWS), :] = (1.0 / scale) * state - factor * total


def local(counts, density, velocity, pressure):
    nx, ny, nz = density.shape
    nrow = nx * ny
    npeers = sum(counts) - len(counts)
    f32 = jnp.float32
    vmem = pl.BlockSpec(memory_space=pltpu.VMEM)
    return pl.pallas_call(
        functools.partial(kernel, counts),
        out_shape=jax.ShapeDtypeStruct((5, nx, ny, nz), f32),
        in_specs=[vmem] * 3,
        out_specs=vmem,
        scratch_shapes=[
            pltpu.VMEM((15, (nx + 6) * ny, nz), f32),
            pltpu.VMEM((15, nx * (ny + 3 * ROWS), nz), f32),
            pltpu.VMEM((15, nz + 3 * ROWS, nrow), f32),
            pltpu.VMEM((5, (nx + 1) * ny, nz), f32),
            pltpu.VMEM((5, nx * (ny + ROWS), nz), f32),
            pltpu.VMEM((5, nz + ROWS, nrow), f32),
            pltpu.VMEM((5, nrow, nz), f32),
            pltpu.VMEM((5, nz, nrow), f32),
            pltpu.VMEM((2, 5, 3, ny, nz), f32),
            pltpu.VMEM((2, 5, nx, ROWS, nz), f32),
            pltpu.VMEM((2, 5, ROWS, nrow), f32),
            pltpu.VMEM((4, ROWS, nz), f32),
            pltpu.VMEM((npeers, ROWS, nz), f32),
            pltpu.SemaphoreType.DMA((14,)),
            pltpu.SemaphoreType.DMA((14,)),
            pltpu.SemaphoreType.DMA((npeers,)),
            pltpu.SemaphoreType.DMA((npeers,)),
        ],
        compiler_params=pltpu.CompilerParams(collective_id=0, has_side_effects=True),
    )(density, velocity, pressure)


def solution(mesh):
    counts = tuple(mesh.shape[a] for a in AXES)
    in_specs = (P("gx", "gy", "gz"), P(None, "gx", "gy", "gz"), P("gx", "gy", "gz"))
    out_specs = P(None, "gx", "gy", "gz")
    return jax.shard_map(
        functools.partial(local, counts), mesh=mesh, in_specs=in_specs, out_specs=out_specs, check_vma=False
    )
```

```python
import functools
import itertools
import math

import jax
import jax.numpy as jnp
from jax import lax
from jax.experimental import pallas as pl
from jax.experimental.pallas import tpu as pltpu
from jax.sharding import PartitionSpec as P

MESH = pl.DeviceIdType.MESH
AXES = ("gx", "gy", "gz")
gamma_gas = 1.4
weno_eps = 1e-06
cfl_number = 0.4
scale = 0.125
eps_outer = 0.75 * 16.0 * scale * scale * weno_eps
eps_inner = 0.75 * 4.0 * scale * scale * weno_eps
ROWS = 8
EARLY = 0


def rcp(x):
    guess = pl.reciprocal(x, approx=True)
    return guess * (2.0 - x * guess)


def cell_basis(rho, v, p):
    inv_root = lax.rsqrt(rho)
    c2 = gamma_gas * p * (inv_root * inv_root)
    m = [rho * u for u in v]
    energy = 2.5 * p + 0.5 * (m[0] * v[0] + m[1] * v[1] + m[2] * v[2])
    return rho, v, p, m, energy, rho * inv_root, c2, c2 * lax.rsqrt(c2)


def cell_arrays(basis, order):
    rho, v, p, m, energy, root, c2, sound = basis
    vn, va, vb = [v[k] for k in order]
    mn, ma, mb = [m[k] for k in order]
    return [
        rho, mn, ma, mb, energy,
        mn * vn + p, ma * vn, mb * vn, (energy + p) * vn,
        root, vn, va, vb, c2, jnp.abs(vn) + sound,
    ]


FIRST, SECOND, THIRD = (0, 1, 2), (1, 0, 2), (2, 0, 1)


def put_cells(ref, row, arrays):
    for k, array in enumerate(arrays):
        ref[k, pl.ds(row, ROWS), :] = array


def weno(d1, d2, d3, d4, eps):
    h2 = (d2 + d2) - d1
    h3 = (d3 + d3) - d4
    e1, e2, e3 = d2 - d1, d3 - d2, d4 - d3
    s2, s3 = 0.75 * d2, 0.75 * d3
    a = (e1 * e1 + s2 * h2) + eps
    b = (e2 * e2 + s2 * d3) + eps
    c = (e3 * e3 + s3 * h3) + eps
    bc, ac, ab = b * c, a * c, a * b
    w0 = bc * bc
    w1 = 6.0 * (ac * ac)
    w2 = 1.5 * (ab * ab)
    den = w0 + w1 + (w2 + w2)
    return (w0 * (h2 - d3) + w2 * (h3 - d2)) * rcp(den)


def face_tile(cells, flux, base, stride, row):
    def load(k, j):
        return cells[k, pl.ds(base + j * stride, ROWS), :]

    sl, sr = load(9, 2), load(9, 3)
    inv = rcp(sl + sr)
    wl, wr = sl * inv, sr * inv
    vl = [load(10 + k, 2) for k in range(3)]
    dv = [load(10 + k, 3) - vl[k] for k in range(3)]
    un, ta, tb = [vl[k] + wr * dv[k] for k in range(3)]
    jump = dv[0] * dv[0] + dv[1] * dv[1] + dv[2] * dv[2]
    c2 = wl * load(13, 2) + wr * load(13, 3) + (0.2 * (wl * wr)) * jump
    ic = lax.rsqrt(c2)
    sound = c2 * ic
    b1 = 0.4 * (ic * ic)
    qh = 0.5 * (un * un + ta * ta + tb * tb)
    enth = 2.5 * c2 + qh
    alpha = load(14, 0)
    for j in range(1, 6):
        alpha = jnp.maximum(alpha, load(14, j))

    state = [[load(k, j) for j in range(6)] for k in range(5)]
    phys = [state[1]] + [[load(k, j) for j in range(6)] for k in range(5, 9)]
    du = [[s[j + 1] - s[j] for j in range(5)] for s in state]
    df = [du[1]] + [[s[j + 1] - s[j] for j in range(5)] for s in phys[1:]]
    au = [[alpha * d for d in s] for s in du]

    def project(r, mn, ma, mb, e):
        s = (un * r - mn) * ic
        z = b1 * (e - un * mn - ta * ma - tb * mb + qh * r)
        return z + s, r - z, ma - ta * r, mb - tb * r, z - s

    plus = [project(*[df[k][j] + au[k][j] for k in range(5)]) for j in range(4)]
    minus = [project(*[df[k][j] - au[k][j] for k in range(5)]) for j in range(1, 5)]
    hats = []
    for k in range(5):
        eps = eps_outer if k in (0, 4) else eps_inner
        up = weno(plus[0][k], plus[1][k], plus[2][k], plus[3][k], eps)
        down = weno(minus[3][k], minus[2][k], minus[1][k], minus[0][k], eps)
        hats.append(up - down)
    lin = []
    for k in range(5):
        centre = 6.0 * (phys[k][2] + phys[k][3]) + (df[k][1] - df[k][3])
        lin.append(centre + ((au[k][1] + au[k][3]) - (au[k][2] + au[k][2])))
    h1, h2, h3, h4, h5 = hats
    h2, h3, h4 = h2 + h2, h3 + h3, h4 + h4
    h15 = h1 + h5
    k5 = sound * (h5 - h1)
    s = h15 + h2
    result = [
        lin[0] + s,
        lin[1] + (un * s + k5),
        lin[2] + (ta * s + h3),
        lin[3] + (tb * s + h4),
        lin[4] + (enth * h15 + un * k5 + qh * h2 + ta * h3 + tb * h4),
    ]
    for k in range(5):
        flux[k, pl.ds(row, ROWS), :] = result[k]


def top_groups(counts):
    if math.prod(counts) <= 64:
        return (tuple(range(len(counts))),)
    return tuple((a,) for a in range(len(counts)))


def kernel(
    counts, early, den_in, vel_in, pre_in, out,
    den, vel, pre, cx, cy, cz, gx, gy, gz, acc, tz, hx, hy, hz, top, got,
    in_sem, send_sem, recv_sem, top_send, top_recv,
):
    nx, ny, lanes = den.shape
    nrow = nx * ny
    nz = lanes
    tiles = ny // ROWS
    ypad = ny + 3 * ROWS
    yface = ny + ROWS

    me = [lax.axis_index(a) for a in AXES]
    barrier = pltpu.get_barrier_semaphore()
    groups = top_groups(counts)
    peers = []
    for stage, group in enumerate(groups):
        for shift in itertools.product(*(range(counts[a]) for a in group)):
            if any(shift):
                peer = {AXES[a]: lax.rem(me[a] + k, counts[a]) for a, k in zip(group, shift)}
                peers.append((stage, peer))
    for _, peer in peers:
        pl.semaphore_signal(barrier, inc=1, device_id=peer, device_id_type=MESH)

    pairs = ((den_in, den), (vel_in, vel), (pre_in, pre))
    loads = [pltpu.make_async_copy(a, b, in_sem.at[k]) for k, (a, b) in enumerate(pairs)]
    for copy in loads:
        copy.start()
    for copy in loads:
        copy.wait()

    def speeds(i, best):
        for t in range(tiles):
            r = t * ROWS
            inv_root = lax.rsqrt(den[i, pl.ds(r, ROWS), :])
            c2 = gamma_gas * pre[i, pl.ds(r, ROWS), :] * (inv_root * inv_root)
            v1, v2, v3 = [jnp.abs(vel[k, i, pl.ds(r, ROWS), :]) for k in range(3)]
            best = jnp.maximum(best, ((v1 + v2) + v3) + 3.0 * (c2 * lax.rsqrt(c2)))
        return best

    best = lax.fori_loop(0, nx, speeds, jnp.zeros((ROWS, lanes), jnp.float32))
    top[0] = jnp.max(best, axis=0, keepdims=True)

    def own_cells():
        @pl.loop(0, nx)
        def _(i):
            for t in range(tiles):
                r = t * ROWS
                rho = scale * den[i, pl.ds(r, ROWS), :]
                p = scale * pre[i, pl.ds(r, ROWS), :]
                basis = cell_basis(rho, [vel[k, i, pl.ds(r, ROWS), :] for k in range(3)], p)
                put_cells(cx, pl.multiple_of((3 + i) * ny + r, ROWS), cell_arrays(basis, FIRST))
                put_cells(cy, pl.multiple_of(i * ypad + ROWS + r, ROWS), cell_arrays(basis, SECOND))

    tz[0] = den[...].reshape(nrow, nz).T
    for k in range(3):
        tz[1 + k] = vel[k].reshape(nrow, nz).T
    tz[4] = pre[...].reshape(nrow, nz).T

    def own_turned():
        @pl.loop(0, nz // ROWS, unroll=4)
        def _(t):
            r = pl.multiple_of(t * ROWS, ROWS)
            rho, v1, v2, v3, p = [tz[k, pl.ds(r, ROWS), :] for k in range(5)]
            basis = cell_basis(scale * rho, (v1, v2, v3), scale * p)
            put_cells(cz, r + ROWS, cell_arrays(basis, THIRD))

    def z_face(t):
        r = pl.multiple_of(t * ROWS, ROWS)
        face_tile(cz, gz, r + 5, 1, r)

    def y_face(i, t):
        face_tile(cy, gy, i * ypad + t * ROWS + 5, 1, pl.multiple_of(i * yface + t * ROWS, ROWS))

    if early >= 1:
        own_cells()
    if early >= 2:
        own_turned()

    pl.semaphore_wait(barrier, len(peers))

    def remote(src, dst, slot, peer):
        copy = pltpu.make_async_remote_copy(
            src_ref=src, dst_ref=dst, send_sem=send_sem.at[slot], recv_sem=recv_sem.at[slot],
            device_id=peer, device_id_type=MESH,
        )
        copy.start()
        return copy

    def send_top(axis):
        copies = []
        for slot, (other, peer) in enumerate(peers):
            if other == axis:
                copy = pltpu.make_async_remote_copy(
                    src_ref=top.at[axis], dst_ref=got.at[slot],
                    send_sem=top_send.at[slot], recv_sem=top_recv.at[slot],
                    device_id=peer, device_id_type=MESH,
                )
                copy.start()
                copies.append((slot, copy))
        return copies

    def take_top(axis, copies):
        best = top[axis]
        for slot, copy in copies:
            copy.wait()
            best = jnp.maximum(best, got[slot])
        top[axis + 1] = best

    def next_top(stage, copies):
        if stage >= len(groups) - 1:
            return copies
        take_top(stage, copies)
        return send_top(stage + 1)

    def near(axis, way):
        return {AXES[axis]: lax.rem(me[axis] + way + counts[axis], counts[axis])}

    pending = send_top(0)
    zc = [
        remote(tz.at[:, pl.ds(nz - ROWS, ROWS), :], hz.at[0], 0, near(2, 1)),
        remote(tz.at[:, pl.ds(0, ROWS), :], hz.at[1], 1, near(2, -1)),
    ]
    yc, xc = [], []
    for side, start, way in ((0, ny - ROWS, 1), (1, 0, -1)):
        peer = near(1, way)
        slot = 2 + 3 * side
        yc.append(remote(den.at[:, pl.ds(start, ROWS), :], hy.at[side, 0], slot, peer))
        yc.append(remote(vel.at[:, :, pl.ds(start, ROWS), :], hy.at[side, pl.ds(1, 3)], slot + 1, peer))
        yc.append(remote(pre.at[:, pl.ds(start, ROWS), :], hy.at[side, 4], slot + 2, peer))
    for side, start, way in ((0, nx - 3, 1), (1, 0, -1)):
        peer = near(0, way)
        slot = 8 + 3 * side
        xc.append(remote(den.at[pl.ds(start, 3)], hx.at[side, 0], slot, peer))
        xc.append(remote(vel.at[:, pl.ds(start, 3)], hx.at[side, pl.ds(1, 3)], slot + 1, peer))
        xc.append(remote(pre.at[pl.ds(start, 3)], hx.at[side, 4], slot + 2, peer))

    if early < 1:
        own_cells()
    if early < 2:
        own_turned()
    pl.loop(1, nz // ROWS - 1)(z_face)
    pending = next_top(0, pending)

    @pl.loop(0, nx * (tiles - 2))
    def _(q):
        y_face(q // (tiles - 2), lax.rem(q, tiles - 2) + 1)

    pending = next_top(1, pending)

    for side, row in ((0, 0), (1, nz + ROWS)):
        zc[side].wait()
        rho, v1, v2, v3, p = [hz[side, k] for k in range(5)]
        put_cells(cz, row, cell_arrays(cell_basis(scale * rho, (v1, v2, v3), scale * p), THIRD))

    @pl.loop(0, 3)
    def _(t):
        z_face(jnp.where(t == 0, 0, nz // ROWS - 2 + t))

    for k, field in enumerate((0, 3, 1, 2, 4)):
        acc[field] = (gz[k, pl.ds(1, nz), :] - gz[k, pl.ds(0, nz), :]).T

    for copy in yc:
        copy.wait()
    for side in range(2):
        for i in range(nx):
            rho, v1, v2, v3, p = [hy[side, k, i] for k in range(5)]
            row = i * ypad + side * (ny + ROWS)
            put_cells(cy, row, cell_arrays(cell_basis(scale * rho, (v1, v2, v3), scale * p), SECOND))

    @pl.loop(0, nx * 3)
    def _(q):
        t = lax.rem(q, 3)
        y_face(q // 3, jnp.where(t == 0, 0, tiles - 2 + t))

    pending = next_top(2, pending)

    for copy in xc:
        copy.wait()
    for side in range(2):
        @pl.loop(0, 3)
        def _(i):
            for t in range(tiles):
                r = t * ROWS
                rho, v1, v2, v3, p = [hx[side, k, i, pl.ds(r, ROWS), :] for k in range(5)]
                row = pl.multiple_of((side * (nx + 3) + i) * ny + r, ROWS)
                put_cells(cx, row, cell_arrays(cell_basis(scale * rho, (v1, v2, v3), scale * p), FIRST))

    @pl.loop(0, (nx + 1) * tiles)
    def _(q):
        r = pl.multiple_of(q * ROWS, ROWS)
        face_tile(cx, gx, r, ny, r)

    take_top(len(groups) - 1, pending)
    largest = jnp.max(top[len(groups)], axis=(0, 1), keepdims=True)
    factor = jnp.broadcast_to((cfl_number / (12.0 * scale)) / largest, (ROWS, lanes))

    @pl.loop(0, nx)
    def _(i):
        for t in range(tiles):
            r = t * ROWS
            row = pl.multiple_of(i * ny + r, ROWS)
            yrow = pl.multiple_of(i * yface + r, ROWS)
            for field, k in enumerate((0, 2, 1, 3, 4)):
                total = acc[field, pl.ds(row, ROWS), :]
                total = total + (gy[k, pl.ds(yrow + 1, ROWS), :] - gy[k, pl.ds(yrow, ROWS), :])
                total = total + (gx[field, pl.ds(row + ny, ROWS), :] - gx[field, pl.ds(row, ROWS), :])
                state = cx[field, pl.ds(pl.multiple_of(row + 3 * ny, ROWS), ROWS), :]
                out[field, i, pl.ds(r, ROWS), :] = (1.0 / scale) * state - factor * total


def local(counts, density, velocity, pressure):
    nx, ny, nz = density.shape
    nrow = nx * ny
    npeers = sum(math.prod(counts[a] for a in group) - 1 for group in top_groups(counts))
    f32 = jnp.float32
    vmem = pl.BlockSpec(memory_space=pltpu.VMEM)
    return pl.pallas_call(
        functools.partial(kernel, counts, EARLY),
        out_shape=pltpu.VMEM((5, nx, ny, nz), f32),
        in_specs=[pl.BlockSpec(memory_space=pl.ANY)] * 3,
        out_specs=vmem,
        scratch_shapes=[
            pltpu.VMEM((nx, ny, nz), f32),
            pltpu.VMEM((3, nx, ny, nz), f32),
            pltpu.VMEM((nx, ny, nz), f32),
            pltpu.VMEM((15, (nx + 6) * ny + ROWS, nz), f32),
            pltpu.VMEM((15, nx * (ny + 3 * ROWS) + ROWS, nz), f32),
            pltpu.VMEM((15, nz + 3 * ROWS, nrow), f32),
            pltpu.VMEM((5, (nx + 1) * ny, nz), f32),
            pltpu.VMEM((5, nx * (ny + ROWS), nz), f32),
            pltpu.VMEM((5, nz + ROWS, nrow), f32),
            pltpu.VMEM((5, nrow, nz), f32),
            pltpu.VMEM((5, nz, nrow), f32),
            pltpu.VMEM((2, 5, 3, ny, nz), f32),
            pltpu.VMEM((2, 5, nx, ROWS, nz), f32),
            pltpu.VMEM((2, 5, ROWS, nrow), f32),
            pltpu.VMEM((4, 1, nz), f32),
            pltpu.VMEM((npeers, 1, nz), f32),
            pltpu.SemaphoreType.DMA((3,)),
            pltpu.SemaphoreType.DMA((14,)),
            pltpu.SemaphoreType.DMA((14,)),
            pltpu.SemaphoreType.DMA((npeers,)),
            pltpu.SemaphoreType.DMA((npeers,)),
        ],
        compiler_params=pltpu.CompilerParams(collective_id=0, has_side_effects=True),
    )(density, velocity, pressure)


def solution(mesh):
    counts = tuple(mesh.shape[a] for a in AXES)
    in_specs = (P("gx", "gy", "gz"), P(None, "gx", "gy", "gz"), P("gx", "gy", "gz"))
    out_specs = P(None, "gx", "gy", "gz")
    return jax.shard_map(
        functools.partial(local, counts), mesh=mesh, in_specs=in_specs, out_specs=out_specs, check_vma=False
    )
```

```python
import functools
import itertools
import math

import jax
import jax.numpy as jnp
from jax import lax
from jax.experimental import pallas as pl
from jax.experimental.pallas import tpu as pltpu
from jax.sharding import PartitionSpec as P

MESH = pl.DeviceIdType.MESH
AXES = ("gx", "gy", "gz")
gamma_gas = 1.4
weno_eps = 1e-06
cfl_number = 0.4
scale = 0.125
eps_outer = 0.75 * 16.0 * scale * scale * weno_eps
eps_inner = 0.75 * 4.0 * scale * scale * weno_eps
ROWS = 8
EARLY = 0


def rcp(x):
    guess = pl.reciprocal(x, approx=True)
    return guess * (2.0 - x * guess)


def cell_basis(rho, v, p):
    inv_root = lax.rsqrt(rho)
    c2 = gamma_gas * p * (inv_root * inv_root)
    m = [rho * u for u in v]
    energy = 2.5 * p + 0.5 * (m[0] * v[0] + m[1] * v[1] + m[2] * v[2])
    return rho, v, p, m, energy, rho * inv_root, c2, c2 * lax.rsqrt(c2)


def cell_arrays(basis, order):
    rho, v, p, m, energy, root, c2, sound = basis
    vn, va, vb = [v[k] for k in order]
    mn, ma, mb = [m[k] for k in order]
    return [
        rho, mn, ma, mb, energy,
        mn * vn + p, ma * vn, mb * vn, (energy + p) * vn,
        root, vn, va, vb, c2, jnp.abs(vn) + sound,
    ]


FIRST, SECOND, THIRD = (0, 1, 2), (1, 0, 2), (2, 0, 1)


def put_cells(ref, row, arrays):
    for k, array in enumerate(arrays):
        ref[k, pl.ds(row, array.shape[0]), :] = array


def weno(d1, d2, d3, d4, eps):
    h2 = (d2 + d2) - d1
    h3 = (d3 + d3) - d4
    e1, e2, e3 = d2 - d1, d3 - d2, d4 - d3
    s2, s3 = 0.75 * d2, 0.75 * d3
    a = (e1 * e1 + s2 * h2) + eps
    b = (e2 * e2 + s2 * d3) + eps
    c = (e3 * e3 + s3 * h3) + eps
    bc, ac, ab = b * c, a * c, a * b
    w0 = bc * bc
    w1 = 6.0 * (ac * ac)
    w2 = 1.5 * (ab * ab)
    den = w0 + w1 + (w2 + w2)
    return (w0 * (h2 - d3) + w2 * (h3 - d2)) * rcp(den)


def face_tile(cells, flux, base, stride, row):
    def load(k, j):
        return cells[k, pl.ds(base + j * stride, ROWS), :]

    sl, sr = load(9, 2), load(9, 3)
    inv = rcp(sl + sr)
    wl, wr = sl * inv, sr * inv
    vl = [load(10 + k, 2) for k in range(3)]
    dv = [load(10 + k, 3) - vl[k] for k in range(3)]
    un, ta, tb = [vl[k] + wr * dv[k] for k in range(3)]
    jump = dv[0] * dv[0] + dv[1] * dv[1] + dv[2] * dv[2]
    c2 = wl * load(13, 2) + wr * load(13, 3) + (0.2 * (wl * wr)) * jump
    ic = lax.rsqrt(c2)
    sound = c2 * ic
    b1 = 0.4 * (ic * ic)
    qh = 0.5 * (un * un + ta * ta + tb * tb)
    enth = 2.5 * c2 + qh
    alpha = load(14, 0)
    for j in range(1, 6):
        alpha = jnp.maximum(alpha, load(14, j))

    state = [[load(k, j) for j in range(6)] for k in range(5)]
    phys = [state[1]] + [[load(k, j) for j in range(6)] for k in range(5, 9)]
    du = [[s[j + 1] - s[j] for j in range(5)] for s in state]
    df = [du[1]] + [[s[j + 1] - s[j] for j in range(5)] for s in phys[1:]]
    au = [[alpha * d for d in s] for s in du]

    def project(r, mn, ma, mb, e):
        s = (un * r - mn) * ic
        z = b1 * (e - un * mn - ta * ma - tb * mb + qh * r)
        return z + s, r - z, ma - ta * r, mb - tb * r, z - s

    plus = [project(*[df[k][j] + au[k][j] for k in range(5)]) for j in range(4)]
    minus = [project(*[df[k][j] - au[k][j] for k in range(5)]) for j in range(1, 5)]
    hats = []
    for k in range(5):
        eps = eps_outer if k in (0, 4) else eps_inner
        up = weno(plus[0][k], plus[1][k], plus[2][k], plus[3][k], eps)
        down = weno(minus[3][k], minus[2][k], minus[1][k], minus[0][k], eps)
        hats.append(up - down)
    lin = []
    for k in range(5):
        centre = 6.0 * (phys[k][2] + phys[k][3]) + (df[k][1] - df[k][3])
        lin.append(centre + ((au[k][1] + au[k][3]) - (au[k][2] + au[k][2])))
    h1, h2, h3, h4, h5 = hats
    h2, h3, h4 = h2 + h2, h3 + h3, h4 + h4
    h15 = h1 + h5
    k5 = sound * (h5 - h1)
    s = h15 + h2
    result = [
        lin[0] + s,
        lin[1] + (un * s + k5),
        lin[2] + (ta * s + h3),
        lin[3] + (tb * s + h4),
        lin[4] + (enth * h15 + un * k5 + qh * h2 + ta * h3 + tb * h4),
    ]
    for k in range(5):
        flux[k, pl.ds(row, ROWS), :] = result[k]


def top_groups(counts):
    if math.prod(counts) <= 64:
        return (tuple(range(len(counts))),)
    return tuple((a,) for a in range(len(counts)))


def kernel(
    counts, early, den_in, vel_in, pre_in, out,
    den, vel, pre, cx, cy, cz, gx, gy, gz, acc, tz, hx, sy, hy, hz, top, got,
    in_sem, send_sem, recv_sem, top_send, top_recv,
):
    nx, ny, lanes = den.shape
    nrow = nx * ny
    nz = lanes
    tiles = ny // ROWS
    ypad = ny + 3 * ROWS
    yface = ny + ROWS

    me = [lax.axis_index(a) for a in AXES]
    barrier = pltpu.get_barrier_semaphore()
    groups = top_groups(counts)
    peers = []
    for stage, group in enumerate(groups):
        for shift in itertools.product(*(range(counts[a]) for a in group)):
            if any(shift):
                peer = {AXES[a]: lax.rem(me[a] + k, counts[a]) for a, k in zip(group, shift)}
                peers.append((stage, peer))
    for _, peer in peers:
        pl.semaphore_signal(barrier, inc=1, device_id=peer, device_id_type=MESH)

    pairs = ((den_in, den), (vel_in, vel), (pre_in, pre))
    loads = [pltpu.make_async_copy(a, b, in_sem.at[k]) for k, (a, b) in enumerate(pairs)]
    for copy in loads:
        copy.start()
    for copy in loads:
        copy.wait()

    def speeds(i, best):
        for t in range(tiles):
            r = t * ROWS
            inv_root = lax.rsqrt(den[i, pl.ds(r, ROWS), :])
            c2 = gamma_gas * pre[i, pl.ds(r, ROWS), :] * (inv_root * inv_root)
            v1, v2, v3 = [jnp.abs(vel[k, i, pl.ds(r, ROWS), :]) for k in range(3)]
            best = jnp.maximum(best, ((v1 + v2) + v3) + 3.0 * (c2 * lax.rsqrt(c2)))
        return best

    best = lax.fori_loop(0, nx, speeds, jnp.zeros((ROWS, lanes), jnp.float32))
    top[0] = jnp.max(best, axis=0, keepdims=True)

    def own_cells():
        @pl.loop(0, nx)
        def _(i):
            for t in range(tiles):
                r = t * ROWS
                rho = scale * den[i, pl.ds(r, ROWS), :]
                p = scale * pre[i, pl.ds(r, ROWS), :]
                basis = cell_basis(rho, [vel[k, i, pl.ds(r, ROWS), :] for k in range(3)], p)
                put_cells(cx, pl.multiple_of((3 + i) * ny + r, ROWS), cell_arrays(basis, FIRST))
                put_cells(cy, pl.multiple_of(i * ypad + ROWS + r, ROWS), cell_arrays(basis, SECOND))

    for side, start in ((0, ny - 3), (1, 0)):
        for i in range(nx):
            rows = [den[i, pl.ds(start, 3), :]]
            rows += [vel[k, i, pl.ds(start, 3), :] for k in range(3)]
            rows.append(pre[i, pl.ds(start, 3), :])
            for k in range(5):
                sy[side, pl.ds(3 * (k * nx + i), 3), :] = rows[k]

    tz[0] = den[...].reshape(nrow, nz).T
    for k in range(3):
        tz[1 + k] = vel[k].reshape(nrow, nz).T
    tz[4] = pre[...].reshape(nrow, nz).T

    def own_turned():
        @pl.loop(0, nz // ROWS, unroll=4)
        def _(t):
            r = pl.multiple_of(t * ROWS, ROWS)
            rho, v1, v2, v3, p = [tz[k, pl.ds(r, ROWS), :] for k in range(5)]
            basis = cell_basis(scale * rho, (v1, v2, v3), scale * p)
            put_cells(cz, r + ROWS, cell_arrays(basis, THIRD))

    def z_face(t):
        r = pl.multiple_of(t * ROWS, ROWS)
        face_tile(cz, gz, r + 5, 1, r)

    def y_face(i, t):
        face_tile(cy, gy, i * ypad + t * ROWS + 5, 1, pl.multiple_of(i * yface + t * ROWS, ROWS))

    if early >= 1:
        own_cells()
    if early >= 2:
        own_turned()

    pl.semaphore_wait(barrier, len(peers))

    def remote(src, dst, slot, peer):
        copy = pltpu.make_async_remote_copy(
            src_ref=src, dst_ref=dst, send_sem=send_sem.at[slot], recv_sem=recv_sem.at[slot],
            device_id=peer, device_id_type=MESH,
        )
        copy.start()
        return copy

    def send_top(axis):
        copies = []
        for slot, (other, peer) in enumerate(peers):
            if other == axis:
                copy = pltpu.make_async_remote_copy(
                    src_ref=top.at[axis], dst_ref=got.at[slot],
                    send_sem=top_send.at[slot], recv_sem=top_recv.at[slot],
                    device_id=peer, device_id_type=MESH,
                )
                copy.start()
                copies.append((slot, copy))
        return copies

    def take_top(axis, copies):
        best = top[axis]
        for slot, copy in copies:
            copy.wait()
            best = jnp.maximum(best, got[slot])
        top[axis + 1] = best

    def next_top(stage, copies):
        if stage >= len(groups) - 1:
            return copies
        take_top(stage, copies)
        return send_top(stage + 1)

    def near(axis, way):
        return {AXES[axis]: lax.rem(me[axis] + way + counts[axis], counts[axis])}

    pending = send_top(0)
    zc = [
        remote(tz.at[:, pl.ds(nz - ROWS, ROWS), :], hz.at[0], 0, near(2, 1)),
        remote(tz.at[:, pl.ds(0, ROWS), :], hz.at[1], 1, near(2, -1)),
    ]
    yc, xc = [], []
    for side, way in ((0, 1), (1, -1)):
        yc.append(remote(sy.at[side], hy.at[side], 2 + side, near(1, way)))
    for side, start, way in ((0, nx - 3, 1), (1, 0, -1)):
        peer = near(0, way)
        slot = 4 + 3 * side
        xc.append(remote(den.at[pl.ds(start, 3)], hx.at[side, 0], slot, peer))
        xc.append(remote(vel.at[:, pl.ds(start, 3)], hx.at[side, pl.ds(1, 3)], slot + 1, peer))
        xc.append(remote(pre.at[pl.ds(start, 3)], hx.at[side, 4], slot + 2, peer))

    if early < 1:
        own_cells()
    if early < 2:
        own_turned()
    pl.loop(1, nz // ROWS - 1)(z_face)
    pending = next_top(0, pending)

    @pl.loop(0, nx * (tiles - 2))
    def _(q):
        y_face(q // (tiles - 2), lax.rem(q, tiles - 2) + 1)

    pending = next_top(1, pending)

    for side, row in ((0, 0), (1, nz + ROWS)):
        zc[side].wait()
        rho, v1, v2, v3, p = [hz[side, k] for k in range(5)]
        put_cells(cz, row, cell_arrays(cell_basis(scale * rho, (v1, v2, v3), scale * p), THIRD))

    @pl.loop(0, 3)
    def _(t):
        z_face(jnp.where(t == 0, 0, nz // ROWS - 2 + t))

    for k, field in enumerate((0, 3, 1, 2, 4)):
        acc[field] = (gz[k, pl.ds(1, nz), :] - gz[k, pl.ds(0, nz), :]).T

    for copy in yc:
        copy.wait()
    for side in range(2):
        for i in range(nx):
            rho, v1, v2, v3, p = [hy[side, pl.ds(3 * (k * nx + i), 3), :] for k in range(5)]
            row = i * ypad + ROWS + (ny if side else -3)
            put_cells(cy, row, cell_arrays(cell_basis(scale * rho, (v1, v2, v3), scale * p), SECOND))

    @pl.loop(0, nx * 3)
    def _(q):
        t = lax.rem(q, 3)
        y_face(q // 3, jnp.where(t == 0, 0, tiles - 2 + t))

    pending = next_top(2, pending)

    for copy in xc:
        copy.wait()
    for side in range(2):
        @pl.loop(0, 3)
        def _(i):
            for t in range(tiles):
                r = t * ROWS
                rho, v1, v2, v3, p = [hx[side, k, i, pl.ds(r, ROWS), :] for k in range(5)]
                row = pl.multiple_of((side * (nx + 3) + i) * ny + r, ROWS)
                put_cells(cx, row, cell_arrays(cell_basis(scale * rho, (v1, v2, v3), scale * p), FIRST))

    @pl.loop(0, (nx + 1) * tiles)
    def _(q):
        r = pl.multiple_of(q * ROWS, ROWS)
        face_tile(cx, gx, r, ny, r)

    take_top(len(groups) - 1, pending)
    largest = jnp.max(top[len(groups)], axis=(0, 1), keepdims=True)
    factor = jnp.broadcast_to((cfl_number / (12.0 * scale)) / largest, (ROWS, lanes))

    @pl.loop(0, nx)
    def _(i):
        for t in range(tiles):
            r = t * ROWS
            row = pl.multiple_of(i * ny + r, ROWS)
            yrow = pl.multiple_of(i * yface + r, ROWS)
            for field, k in enumerate((0, 2, 1, 3, 4)):
                total = acc[field, pl.ds(row, ROWS), :]
                total = total + (gy[k, pl.ds(yrow + 1, ROWS), :] - gy[k, pl.ds(yrow, ROWS), :])
                total = total + (gx[field, pl.ds(row + ny, ROWS), :] - gx[field, pl.ds(row, ROWS), :])
                state = cx[field, pl.ds(pl.multiple_of(row + 3 * ny, ROWS), ROWS), :]
                out[field, i, pl.ds(r, ROWS), :] = (1.0 / scale) * state - factor * total


def local(counts, density, velocity, pressure):
    nx, ny, nz = density.shape
    nrow = nx * ny
    npeers = sum(math.prod(counts[a] for a in group) - 1 for group in top_groups(counts))
    f32 = jnp.float32
    vmem = pl.BlockSpec(memory_space=pltpu.VMEM)
    return pl.pallas_call(
        functools.partial(kernel, counts, EARLY),
        out_shape=pltpu.VMEM((5, nx, ny, nz), f32),
        in_specs=[pl.BlockSpec(memory_space=pl.ANY)] * 3,
        out_specs=vmem,
        scratch_shapes=[
            pltpu.VMEM((nx, ny, nz), f32),
            pltpu.VMEM((3, nx, ny, nz), f32),
            pltpu.VMEM((nx, ny, nz), f32),
            pltpu.VMEM((15, (nx + 6) * ny + ROWS, nz), f32),
            pltpu.VMEM((15, nx * (ny + 3 * ROWS) + ROWS, nz), f32),
            pltpu.VMEM((15, nz + 3 * ROWS, nrow), f32),
            pltpu.VMEM((5, (nx + 1) * ny, nz), f32),
            pltpu.VMEM((5, nx * (ny + ROWS), nz), f32),
            pltpu.VMEM((5, nz + ROWS, nrow), f32),
            pltpu.VMEM((5, nrow, nz), f32),
            pltpu.VMEM((5, nz, nrow), f32),
            pltpu.VMEM((2, 5, 3, ny, nz), f32),
            pltpu.VMEM((2, pl.cdiv(15 * nx, ROWS) * ROWS, nz), f32),
            pltpu.VMEM((2, pl.cdiv(15 * nx, ROWS) * ROWS, nz), f32),
            pltpu.VMEM((2, 5, ROWS, nrow), f32),
            pltpu.VMEM((4, 1, nz), f32),
            pltpu.VMEM((npeers, 1, nz), f32),
            pltpu.SemaphoreType.DMA((3,)),
            pltpu.SemaphoreType.DMA((10,)),
            pltpu.SemaphoreType.DMA((10,)),
            pltpu.SemaphoreType.DMA((npeers,)),
            pltpu.SemaphoreType.DMA((npeers,)),
        ],
        compiler_params=pltpu.CompilerParams(collective_id=0, has_side_effects=True),
    )(density, velocity, pressure)


def solution(mesh):
    counts = tuple(mesh.shape[a] for a in AXES)
    in_specs = (P("gx", "gy", "gz"), P(None, "gx", "gy", "gz"), P("gx", "gy", "gz"))
    out_specs = P(None, "gx", "gy", "gz")
    return jax.shard_map(
        functools.partial(local, counts), mesh=mesh, in_specs=in_specs, out_specs=out_specs, check_vma=False
    )
```
